32 devices in a mesh: shard: 8 (over z, y), tensor: 2 (over core), context: 2 (over x).
Axes of the slice: x: 2, y: 2, z: 4, core: 2. Of those that a mesh axis runs over, the one named last changes fastest.
Arguments:
- hidden_in: bfloat16 [16, 1024, 1280], P(('shard', 'tensor'), 'context'), may hold values from -6 to 6
- patch_rows: int32 [16, 1024], P('shard', 'context'), may hold values from 0 to 63
- patch_cols: int32 [16, 1024], P('shard', 'context'), may hold values from 0 to 63
- attn_norm_gain: float32 [1280], replicated, may hold values from 0.5 to 1.5
- attn_norm_bias: float32 [1280], replicated, may hold values from -1.2 to 1.2
- query_key_value_weight: bfloat16 [1280, 3, 1280], P(('shard', 'context'), None, 'tensor'), may hold values from -0.15625 to 0.15625
- query_key_value_bias: float32 [3, 1280], replicated, may hold values from -1.2 to 1.2
- out_weight: bfloat16 [1280, 1280], P('tensor', ('shard', 'context')), may hold values from -2.5 to 2.5
- out_bias: float32 [1280], replicated, may hold values from -1.2 to 1.2
- mlp_norm_gain: float32 [1280], replicated, may hold values from 0.5 to 1.5
- mlp_norm_bias: float32 [1280], replicated, may hold values from -1.2 to 1.2
- fc1_weight: bfloat16 [1280, 5120], P(('shard', 'context'), 'tensor'), may hold values from -0.15625 to 0.15625
- fc1_bias: float32 [5120], replicated, may hold values from -1.2 to 1.2
- fc2_weight: bfloat16 [5120, 1280], P('tensor', ('shard', 'context')), may hold values from -0.078125 to 0.078125
- fc2_bias: float32 [1280], replicated, may hold values from -1.2 to 1.2
- cotangent: bfloat16 [16, 1024, 1280], P(('shard', 'tensor'), 'context'), may hold values from -6 to 6
Outputs:
- block_out: bfloat16 [16, 1024, 1280], P(('shard', 'tensor'), 'context')
- grad_input: float32 [16, 1024, 1280], P(('shard', 'tensor'), 'context')
- grad_attn_norm_gain: float32 [1280], replicated
- grad_attn_norm_bias: float32 [1280], replicated
- grad_qkv_weight: float32 [1280, 3, 1280], P(('shard', 'context'), None, 'tensor')
- grad_qkv_bias: float32 [3, 1280], replicated
- grad_out_weight: float32 [1280, 1280], P('tensor', ('shard', 'context'))
- grad_out_bias: float32 [1280], replicated
- grad_mlp_norm_gain: float32 [1280], replicated
- grad_mlp_norm_bias: float32 [1280], replicated
- grad_fc1_weight: float32 [1280, 5120], P(('shard', 'context'), 'tensor')
- grad_fc1_bias: float32 [5120], replicated
- grad_fc2_weight: float32 [5120, 1280], P('tensor', ('shard', 'context'))
- grad_fc2_bias: float32 [1280], replicated
The draws below stay inside these ranges and needn't reach their ends.
All inputs are finite; a program needn't handle non-finite values.
Results may differ from the reference program's by a relative error of at most 0.015.
Values may be sent and summed in bfloat16 or wider, within the bound.
A program may use at most 192 MiB of HBM per device.

```python
from functools import partial
import jax
import jax.numpy as jnp
from jax import lax

D = 1280
HEADS = 16
HEAD_DIM = 80
FF = 5120
PATCHES = 1024
IMAGES = 16


def plant(drawn, stream_key, least, top_value):
    place = [jax.random.randint(jax.random.fold_in(stream_key, axis), (), 0, length) for axis, length in enumerate(drawn.shape)]
    longest = drawn.shape.index(max(drawn.shape))
    beside = place[:longest] + [(place[longest] + 1) % drawn.shape[longest]] + place[longest + 1:]
    return drawn.at[tuple(place)].set(least).at[tuple(beside)].set(top_value)


def strengthened(entries, own_key, source, target, blocks, factor):
    def block_of(position):
        return (jnp.arange(entries.shape[position]) // (entries.shape[position] // blocks)).reshape((-1,) + (1,) * (entries.ndim - 1 - position))

    one_side = jax.random.permutation(own_key, blocks)[block_of(target)]
    far = (block_of(target) + blocks // 2) % blocks
    return jnp.where((block_of(source) == one_side) | (block_of(source) == far), factor * entries, entries)


def block_levels(key, extent, split, least, largest):
    def one(position, blocks):
        heights = jax.random.uniform(jax.random.fold_in(jax.random.fold_in(key, 6), position), (blocks,), jnp.float32, least / len(split), largest / len(split))
        return jnp.repeat(jnp.exp(heights), extent[position] // blocks).reshape((-1,) + (1,) * (len(extent) - position - 1))

    loudness = one(*split[0])
    for cut in split[1:]:
        loudness = loudness * one(*cut)
    return loudness


def normal_values(stream_key, extent, spread, limit, cuts=(), kind=jnp.bfloat16):
    result = spread * jax.random.normal(stream_key, extent, jnp.float32)
    if cuts:
        result = result * block_levels(stream_key, extent, cuts, -0.22, 0.18)
    return jnp.clip(result, -limit, limit).astype(kind)


def bell_draw_with(stream_key, shape, width, most, shards, heavy, kind=jnp.bfloat16):
    result = width * jax.random.normal(stream_key, shape, jnp.float32)
    if shards:
        result = result * block_levels(stream_key, shape, shards, -0.22, 0.18)
    return jnp.clip(strengthened(result, jax.random.fold_in(stream_key, 3), *heavy), -most, most).astype(kind)


def setup_inputs(seed: int = 0) -> dict:
    key_list = jax.random.split(jax.random.key(seed), 17)
    hidden_in = normal_values(key_list[0], (IMAGES, PATCHES, D), 1.0, 6.0, ((0, 16), (1, 2)))
    patch_rows = plant(jax.random.randint(key_list[1], (IMAGES, PATCHES), 0, 64), jax.random.fold_in(key_list[1], 1), 0, 63).astype(jnp.int32)
    patch_cols = plant(jax.random.randint(key_list[2], (IMAGES, PATCHES), 0, 64), jax.random.fold_in(key_list[2], 1), 0, 63).astype(jnp.int32)
    attn_norm_gain = jnp.clip(1.0 + 0.1 * jax.random.normal(key_list[3], (D,), jnp.float32), 0.5, 1.5)
    attn_norm_bias = normal_values(key_list[4], (D,), 0.3, 1.2, (), jnp.float32)
    query_key_value_weight = normal_values(key_list[5], (D, 3, D), D ** -0.5, 0.15625, ((0, 16), (2, 2)))
    query_key_value_bias = normal_values(key_list[6], (3, D), 0.3, 1.2, (), jnp.float32)
    out_weight = normal_values(key_list[7], (D, D), (max(D // 256, 1)) ** -0.5, 2.5, ((0, 2), (1, 16)))
    out_bias = normal_values(key_list[8], (D,), 0.3, 1.2, (), jnp.float32)
    mlp_norm_gain = jnp.clip(1.0 + 0.1 * jax.random.normal(key_list[9], (D,), jnp.float32), 0.5, 1.5)
    mlp_norm_bias = normal_values(key_list[10], (D,), 0.3, 1.2, (), jnp.float32)
    fc1_weight = normal_values(key_list[11], (D, FF), D ** -0.5, 0.15625, ((0, 16), (1, 2)))
    fc1_bias = normal_values(key_list[12], (FF,), 0.3, 1.2, (), jnp.float32)
    fc2_weight = normal_values(key_list[13], (FF, D), FF ** -0.5, 0.078125, ((0, 2), (1, 16)))
    fc2_bias = normal_values(key_list[14], (D,), 0.3, 1.2, (), jnp.float32)
    cotangent = bell_draw_with(key_list[15], (IMAGES, PATCHES, D), 1.0, 6.0, ((0, 16), (1, 2)), (0, 2, 16, 2.0))
    return {"hidden_in": hidden_in, "patch_rows": patch_rows, "patch_cols": patch_cols, "attn_norm_gain": attn_norm_gain, "attn_norm_bias": attn_norm_bias, "query_key_value_weight": query_key_value_weight, "query_key_value_bias": query_key_value_bias, "out_weight": out_weight, "out_bias": out_bias, "mlp_norm_gain": mlp_norm_gain, "mlp_norm_bias": mlp_norm_bias, "fc1_weight": fc1_weight, "fc1_bias": fc1_bias, "fc2_weight": fc2_weight, "fc2_bias": fc2_bias, "cotangent": cotangent}


@jax.custom_vjp
def low(v):
    return lax.optimization_barrier(v.astype(jnp.bfloat16)).astype(jnp.float32)

@jax.custom_vjp
def low_back(v):
    return v

def low_keep(v):
    return (low(v), None)

def low_pass(kept, grad):
    return (grad,)

def back_keep(v):
    return (v, None)

def back_low(kept, grad):
    return (low(grad),)
low.defvjp(low_keep, low_pass)
low_back.defvjp(back_keep, back_low)
highest_precision_setting = lax.Precision.HIGHEST

def layer_norm(field, gain, shift):
    mean_value = lax.optimization_barrier(jnp.mean(field, axis=-1, keepdims=True))
    centered = field - mean_value
    variance = lax.optimization_barrier(jnp.mean(centered * centered, axis=-1, keepdims=True))
    return centered * lax.rsqrt(variance + 1e-06) * gain + shift

def rotary_tables(rows_index, cols_index):
    quarter = HEAD_DIM // 4
    frequency = 10000.0 ** (-jnp.arange(quarter, dtype=jnp.float32) / quarter)
    row_angles = rows_index.astype(jnp.float32)[..., None] * frequency
    col_angles = cols_index.astype(jnp.float32)[..., None] * frequency
    angles = jnp.concatenate([row_angles, col_angles, row_angles, col_angles], axis=-1)
    return (jnp.cos(angles)[:, :, None, :], jnp.sin(angles)[:, :, None, :])

def rotate(field, cosine, sine):
    middle_index = field.shape[-1] // 2
    turned = jnp.concatenate([-field[..., middle_index:], field[..., :middle_index]], axis=-1)
    return field * cosine + turned * sine

def attend_image(inputs):
    queries, keys, values = inputs
    scores = jnp.einsum('phd,khd->hpk', queries, keys, precision=highest_precision_setting) * HEAD_DIM ** (-0.5)
    scores = low_back(scores)
    weights = low(jax.nn.softmax(scores, axis=-1))
    return jnp.einsum('hpk,khd->phd', weights, values, precision=highest_precision_setting)

def layer_forward(cosine, sine, hidden, attn_norm_gain, attn_norm_bias, query_key_value_weight, query_key_value_bias, out_weight, out_bias, mlp_norm_gain, mlp_norm_bias, fc1_weight, fc1_bias, fc2_weight, fc2_bias):
    images, patches, features = hidden.shape
    normalized_input = low(layer_norm(hidden, attn_norm_gain, attn_norm_bias))
    projection_output = jnp.einsum('bxv,vhl->bxhl', normalized_input, query_key_value_weight, precision=highest_precision_setting) + query_key_value_bias
    projection_output = low_back(projection_output)
    head_shape = (images, patches, HEADS, HEAD_DIM)
    queries = low(rotate(projection_output[:, :, 0].reshape(head_shape), cosine, sine))
    keys = low(rotate(projection_output[:, :, 1].reshape(head_shape), cosine, sine))
    values = low(projection_output[:, :, 2].reshape(head_shape))
    mixed = lax.map(jax.checkpoint(attend_image), (queries, keys, values))
    mixed = low(low_back(mixed.reshape(images, patches, features)))
    attn_branch = low_back(jnp.einsum('npe,ed->npd', mixed, out_weight, precision=highest_precision_setting))
    middle = hidden + attn_branch + out_bias
    mlp_normed = low(layer_norm(middle, mlp_norm_gain, mlp_norm_bias))
    pre_act = low_back(jnp.einsum('npd,df->npf', mlp_normed, fc1_weight, precision=highest_precision_setting) + fc1_bias)
    activated = low(pre_act * jax.nn.sigmoid(1.702 * pre_act))
    mlp_branch = low_back(jnp.einsum('npf,fd->npd', activated, fc2_weight, precision=highest_precision_setting))
    return middle + mlp_branch + fc2_bias

def reference(hidden_in, patch_rows, patch_cols, attn_norm_gain, attn_norm_bias, query_key_value_weight, query_key_value_bias, out_weight, out_bias, mlp_norm_gain, mlp_norm_bias, fc1_weight, fc1_bias, fc2_weight, fc2_bias, cotangent):
    cosine, sine = rotary_tables(patch_rows, patch_cols)
    forward = partial(layer_forward, cosine, sine)
    output, pullback = jax.vjp(forward, hidden_in.astype(jnp.float32), attn_norm_gain.astype(jnp.float32), attn_norm_bias.astype(jnp.float32), query_key_value_weight.astype(jnp.float32), query_key_value_bias.astype(jnp.float32), out_weight.astype(jnp.float32), out_bias.astype(jnp.float32), mlp_norm_gain.astype(jnp.float32), mlp_norm_bias.astype(jnp.float32), fc1_weight.astype(jnp.float32), fc1_bias.astype(jnp.float32), fc2_weight.astype(jnp.float32), fc2_bias.astype(jnp.float32))
    grads = pullback(cotangent.astype(jnp.float32))
    return (output.astype(jnp.bfloat16), grads[0], grads[1], grads[2], grads[3], grads[4], grads[5], grads[6], grads[7], grads[8], grads[9], grads[10], grads[11], grads[12])
```

```python
import functools
import math

import jax
import jax.numpy as jnp
from jax import lax
from jax.experimental import pallas as pl
from jax.experimental.pallas import tpu as pltpu
from jax.sharding import PartitionSpec as P

HEAD_DIM = 80
SCALE = HEAD_DIM**-0.5
LOG2E = math.log2(math.e)
BF = jnp.bfloat16
F32 = jnp.float32
PAIR = [(0, 1), (1, 0)]


def dot(a, b, dims):
    return lax.dot_general(a, b, (dims, ((), ())), preferred_element_type=F32)


def grid_of(shards):
    return shards // 2, 2


def use_rings(rows, shards):
    return shards == 8 and rows % 16 == 0


class Net:
    def __init__(self, shards, rows):
        self.shards, self.rows = shards, rows
        self.rings = use_rings(rows, shards)
        self.outer, self.inner = grid_of(shards)
        s = lax.axis_index("shard")
        self.pos = {"z": s // self.inner, "y": s % self.inner, "x": lax.axis_index("context")}
        self.dim = {"z": 0, "y": 1, "x": 2}
        inner, outer = self.inner, self.outer
        self.up = [
            (z * inner + y, ((z + 1) % outer) * inner + y)
            for z in range(outer)
            for y in range(inner)
        ]
        self.side = [(i, i ^ 1) for i in range(shards)]

    def hop(self, block, axis):
        if axis == "x":
            return lax.ppermute(block, "context", PAIR)
        return lax.ppermute(block, "shard", self.side if axis == "y" else self.up)

    def gather(self, piece, order):
        rows, columns = piece.shape
        if not self.rings:
            return lax.all_gather(piece, ("shard", "context"), axis=0, tiled=True)
        block = piece.reshape(1, 1, 1, rows, columns)
        for axis in order:
            dim, here = self.dim[axis], self.pos[axis]
            if axis == "z":
                parts = [block]
                for _ in range(self.outer - 1):
                    parts.append(self.hop(parts[-1], axis))
                slots = []
                for j in range(self.outer):
                    chosen = parts[0]
                    back = (here - j) % self.outer
                    for k in range(1, self.outer):
                        chosen = jnp.where(back == k, parts[k], chosen)
                    slots.append(chosen)
                block = jnp.concatenate(slots, axis=dim)
            else:
                other = self.hop(block, axis)
                first = here == 0
                block = jnp.concatenate(
                    [jnp.where(first, block, other), jnp.where(first, other, block)], axis=dim
                )
        return block.reshape(-1, columns)

    def scatter(self, total, order):
        columns = total.shape[1]
        if not self.rings:
            return lax.psum_scatter(
                total.astype(F32), ("shard", "context"), scatter_dimension=0, tiled=True
            )
        block = total.reshape(self.outer, self.inner, 2, self.rows, columns)
        for axis in order:
            dim, here = self.dim[axis], self.pos[axis]

            def part(index, block=block, dim=dim):
                return lax.dynamic_slice_in_dim(block, index, 1, dim)

            if axis == "z":
                moving = part((here - 1) % self.outer)
                for k in range(2, self.outer + 1):
                    came = self.hop(moving.astype(BF), axis)
                    moving = part((here - k) % self.outer).astype(F32) + came.astype(F32)
                block = moving
            else:
                came = self.hop(part(1 - here).astype(BF), axis)
                block = part(here).astype(F32) + came.astype(F32)
        return block.reshape(self.rows, columns).astype(F32)

    def total(self, vector):
        if not self.rings:
            return lax.psum(vector, ("shard", "tensor", "context"))
        vector = vector + lax.ppermute(vector, "tensor", PAIR)
        vector = vector + lax.ppermute(vector, "context", PAIR)
        step = 1
        while step < self.shards:
            vector = vector + lax.ppermute(
                vector, "shard", [(i, i ^ step) for i in range(self.shards)]
            )
            step *= 2
        return vector


def across(block):
    return lax.ppermute(block, "tensor", PAIR)


def turn(block):
    return lax.ppermute(block, ("tensor", "context"), [(0, 0), (1, 2), (2, 1), (3, 3)])


def rotated(w, cosine, sine):
    half = HEAD_DIM // 2
    a, b = w[:half], w[half:]
    c1, c2, s1, s2 = cosine[:half], cosine[half:], sine[:half], sine[half:]
    return jnp.concatenate([a * c1 - b * s1, b * c2 + a * s2], axis=0)


def rotated_back(w, cosine, sine):
    half = HEAD_DIM // 2
    a, b = w[:half], w[half:]
    c1, c2, s1, s2 = cosine[:half], cosine[half:], sine[:half], sine[half:]
    return jnp.concatenate([a * c1 + b * s2, b * c2 - a * s1], axis=0)


def forward_kernel(tile, pq, pk, pv, cosine, sine, q_out, k_out, v_out, mixed_out, log_out):
    c, s = cosine[...], sine[...]
    keys = rotated(pk[0], c, s).astype(BF)
    queries = rotated(pq[0], c, s).astype(BF)
    values = pv[0].astype(BF)
    q_out[0], k_out[0], v_out[0] = queries, keys, values
    for i in range(queries.shape[1] // tile):
        cols = slice(i * tile, (i + 1) * tile)
        scores = dot(keys, queries[:, cols], ((0,), (0,))) * (SCALE * LOG2E)
        top = jnp.max(scores, axis=0, keepdims=True)
        expos = jnp.exp2(scores - top)
        total = jnp.sum(expos, axis=0, keepdims=True)
        mixed = dot(values, expos.astype(BF), ((1,), (0,))) / total
        mixed_out[0, :, cols] = mixed.astype(BF)
        log_out[0, :, cols] = top + jnp.log2(total)


def backward_kernel(tile, q, k, v, g, log_total, cosine, sine, dq_out, dk_out, dv_out, dk, dv):
    c, s = cosine[...], sine[...]
    keys, values = k[0], v[0]
    dk[...] = jnp.zeros_like(dk)
    dv[...] = jnp.zeros_like(dv)
    for i in range(keys.shape[1] // tile):
        cols = slice(i * tile, (i + 1) * tile)
        queries, grads = q[0, :, cols], g[0, :, cols]
        scores = dot(keys, queries, ((0,), (0,))) * (SCALE * LOG2E)
        probs = jnp.exp2(scores - log_total[0, :, cols])
        grad_probs = dot(values, grads, ((0,), (0,)))
        inner = jnp.sum(probs * grad_probs, axis=0, keepdims=True)
        grad_scores = (probs * (grad_probs - inner)).astype(BF)
        dv[...] += dot(grads, probs.astype(BF), ((1,), (1,)))
        dk[...] += dot(queries, grad_scores, ((1,), (1,)))
        grad_q = dot(keys, grad_scores, ((1,), (0,))) * SCALE
        dq_out[0, :, cols] = rotated_back(grad_q, c[:, cols], s[:, cols]).astype(BF)
    dk_out[0] = rotated_back(dk[...] * SCALE, c, s).astype(BF)
    dv_out[0] = dv[...].astype(BF)


def head_spec(rows, tokens):
    return pl.BlockSpec((1, rows, tokens), lambda h: (h, 0, 0))


def attend_forward(pq, pk, pv, cosine, sine):
    heads, _, tokens = pq.shape
    block, line = head_spec(HEAD_DIM, tokens), head_spec(1, tokens)
    table = pl.BlockSpec((HEAD_DIM, tokens), lambda h: (0, 0))
    low = jax.ShapeDtypeStruct(pq.shape, BF)
    return pl.pallas_call(
        functools.partial(forward_kernel, 256),
        grid=(heads,),
        in_specs=[block] * 3 + [table] * 2,
        out_specs=[block] * 4 + [line],
        out_shape=[low] * 4 + [jax.ShapeDtypeStruct((heads, 1, tokens), F32)],
        compiler_params=pltpu.CompilerParams(vmem_limit_bytes=40 << 20),
        cost_estimate=pl.CostEstimate(
            flops=4 * heads * tokens * tokens * 256,
            bytes_accessed=heads * tokens * HEAD_DIM * 20,
            transcendentals=heads * tokens * tokens,
        ),
        name="attend_forward",
    )(pq, pk, pv, cosine, sine)


def attend_backward(q, k, v, g, log_total, cosine, sine):
    heads, _, tokens = q.shape
    block, line = head_spec(HEAD_DIM, tokens), head_spec(1, tokens)
    table = pl.BlockSpec((HEAD_DIM, tokens), lambda h: (0, 0))
    low = jax.ShapeDtypeStruct(q.shape, BF)
    return pl.pallas_call(
        functools.partial(backward_kernel, 256),
        grid=(heads,),
        in_specs=[block] * 4 + [line] + [table] * 2,
        out_specs=[block] * 3,
        out_shape=[low] * 3,
        scratch_shapes=[pltpu.VMEM((HEAD_DIM, tokens), F32)] * 2,
        compiler_params=pltpu.CompilerParams(vmem_limit_bytes=40 << 20),
        cost_estimate=pl.CostEstimate(
            flops=10 * heads * tokens * tokens * 256,
            bytes_accessed=heads * tokens * HEAD_DIM * 14,
            transcendentals=heads * tokens * tokens,
        ),
        name="attend_backward",
    )(q, k, v, g, log_total, cosine, sine)


def normalize(field, gain, shift):
    centered = field - jnp.mean(field, axis=-1, keepdims=True)
    variance = jnp.mean(centered * centered, axis=-1, keepdims=True)
    inv_scale = lax.rsqrt(variance + 1e-06)
    unit = centered * inv_scale
    return (unit * gain + shift).astype(BF), unit, inv_scale


def norm_backward(grad_normed, unit, inv_scale, gain):
    grad_unit = grad_normed * gain
    mean_grad = jnp.mean(grad_unit, axis=-1, keepdims=True)
    mean_along = jnp.mean(grad_unit * unit, axis=-1, keepdims=True)
    return (
        inv_scale * (grad_unit - mean_grad - unit * mean_along),
        jnp.sum(grad_normed * unit, axis=0),
        jnp.sum(grad_normed, axis=0),
    )


def both(own):
    return jnp.concatenate([own, across(own)], axis=0)


def own_sum(partial):
    half = partial.shape[0] // 2
    return partial[:half].astype(F32) + across(partial[half:]).astype(F32)


def on_device(
    shards,
    hidden_in,
    patch_rows,
    patch_cols,
    attn_norm_gain,
    attn_norm_bias,
    query_key_value_weight,
    query_key_value_bias,
    out_weight,
    out_bias,
    mlp_norm_gain,
    mlp_norm_bias,
    fc1_weight,
    fc1_bias,
    fc2_weight,
    fc2_bias,
    cotangent,
):
    rows, _, width = query_key_value_weight.shape
    units = fc1_weight.shape[1]
    heads = width // HEAD_DIM
    t, c = lax.axis_index("tensor"), lax.axis_index("context")
    net = Net(shards, rows)

    qkv_piece = query_key_value_weight.reshape(rows, 3 * width)
    q_w = net.gather(qkv_piece[:, :width], "zyx")
    k_w = net.gather(qkv_piece[:, width : 2 * width], "zxy")
    v_w = net.gather(qkv_piece[:, 2 * width :], "yxz")
    out_w = net.gather(out_weight.T, "xyz")
    cut = units // 2
    fc1_a = net.gather(fc1_weight[:, :cut], "zyx")
    fc1_b = net.gather(fc1_weight[:, cut:], "zxy")
    fc2_t = fc2_weight.T
    fc2_a = net.gather(fc2_t[:, :cut], "zyx")
    fc2_b = net.gather(fc2_t[:, cut:], "zxy")

    resid = turn(hidden_in[0]).astype(F32)
    grad_low = turn(cotangent[0])
    places = jnp.stack([patch_rows, patch_cols])
    mine = lax.dynamic_index_in_dim(places, c, 1, keepdims=False)
    theirs = lax.ppermute(
        lax.dynamic_index_in_dim(places, 1 - c, 1, keepdims=False), "context", PAIR
    )
    places = jnp.concatenate(
        [jnp.where(t == c, mine, theirs), jnp.where(t == c, theirs, mine)], axis=1
    ).astype(F32)
    quarter = HEAD_DIM // 4
    frequency = 10000.0 ** (-jnp.arange(quarter, dtype=F32) / quarter)
    angles = (places[:, None, :] * frequency[None, :, None]).reshape(2 * quarter, -1)
    cosine, sine = jnp.cos(angles), jnp.sin(angles)
    cosine, sine = jnp.concatenate([cosine] * 2), jnp.concatenate([sine] * 2)

    normed_one, unit_one, scale_one = normalize(resid, attn_norm_gain, attn_norm_bias)
    normed_one = both(normed_one)
    tokens = normed_one.shape[0]
    qkv_bias = lax.dynamic_slice_in_dim(query_key_value_bias, t * width, width, 1)

    def project(weight, bias):
        return (dot(weight, normed_one, ((0,), (1,))) + bias[:, None]).reshape(
            heads, HEAD_DIM, tokens
        )

    queries, keys, values, mixed, log_total = attend_forward(
        project(q_w, qkv_bias[0]),
        project(k_w, qkv_bias[1]),
        project(v_w, qkv_bias[2]),
        cosine,
        sine,
    )
    mixed = mixed.reshape(width, tokens)
    middle = resid + own_sum(dot(mixed, out_w, ((0,), (1,))).astype(BF)) + out_bias
    normed_two, unit_two, scale_two = normalize(middle, mlp_norm_gain, mlp_norm_bias)
    normed_two = both(normed_two)
    own_fc1_bias = lax.dynamic_slice_in_dim(fc1_bias, t * units, units, 0)

    def hidden(weight, bias):
        pre = dot(normed_two, weight, ((1,), (0,))) + bias
        gate = jax.nn.sigmoid(1.702 * pre)
        return (pre * gate).astype(BF), (gate + 1.702 * pre * gate * (1.0 - gate)).astype(BF)

    act_a, slope_a = hidden(fc1_a, own_fc1_bias[:cut])
    act_b, slope_b = hidden(fc1_b, own_fc1_bias[cut:])

    fc2_bias_part = jnp.sum(grad_low.astype(F32), axis=0)
    grad_both = both(grad_low)
    dfc2_a = net.scatter(dot(grad_both, act_a, ((0,), (0,))).astype(BF), "xyz")
    dfc2_b = net.scatter(dot(grad_both, act_b, ((0,), (0,))).astype(BF), "yxz")
    mlp = dot(act_a, fc2_a, ((1,), (1,))) + dot(act_b, fc2_b, ((1,), (1,)))
    block_out = middle + own_sum(mlp.astype(BF)) + fc2_bias
    block_out = turn(block_out.astype(BF))[None]

    grad_pre_a = (dot(grad_both, fc2_a, ((1,), (0,))) * slope_a.astype(F32)).astype(BF)
    grad_pre_b = (dot(grad_both, fc2_b, ((1,), (0,))) * slope_b.astype(F32)).astype(BF)
    back = dot(grad_pre_a, fc1_a, ((1,), (1,))) + dot(grad_pre_b, fc1_b, ((1,), (1,)))
    grad_normed_two = own_sum(back.astype(BF))
    dfc1_a = net.scatter(dot(normed_two, grad_pre_a, ((0,), (0,))).astype(BF), "xyz")
    dfc1_b = net.scatter(dot(normed_two, grad_pre_b, ((0,), (0,))).astype(BF), "yxz")
    fc1_bias_own = jnp.concatenate(
        [jnp.sum(grad_pre_a, axis=0, dtype=F32), jnp.sum(grad_pre_b, axis=0, dtype=F32)]
    )
    grad_norm, gain_two, shift_two = norm_backward(
        grad_normed_two, unit_two, scale_two, mlp_norm_gain
    )
    grad_middle = grad_low.astype(F32) + grad_norm
    out_bias_part = jnp.sum(grad_middle, axis=0)
    mid_both = both(grad_middle.astype(BF))
    grad_mixed = dot(out_w, mid_both, ((0,), (1,))).astype(BF)
    dout = net.scatter(dot(mid_both, mixed, ((0,), (1,))).astype(BF), "xyz")

    dq, dk, dv = attend_backward(
        queries,
        keys,
        values,
        grad_mixed.reshape(heads, HEAD_DIM, tokens),
        log_total,
        cosine,
        sine,
    )
    dq, dk, dv = (g.reshape(width, tokens) for g in (dq, dk, dv))
    dw_q = net.scatter(dot(normed_one, dq, ((0,), (1,))).astype(BF), "xyz")
    dw_k = net.scatter(dot(normed_one, dk, ((0,), (1,))).astype(BF), "yxz")
    dw_v = net.scatter(dot(normed_one, dv, ((0,), (1,))).astype(BF), "zxy")
    back = (
        dot(dq, q_w, ((0,), (1,))) + dot(dk, k_w, ((0,), (1,))) + dot(dv, v_w, ((0,), (1,)))
    )
    grad_norm, gain_one, shift_one = norm_backward(
        own_sum(back.astype(BF)), unit_one, scale_one, attn_norm_gain
    )
    grad_input = turn((grad_middle + grad_norm).astype(BF)).astype(F32)[None]
    qkv_bias_own = jnp.stack([jnp.sum(g, axis=1, dtype=F32) for g in (dq, dk, dv)])
    qkv_slot = lax.dynamic_update_slice_in_dim(
        jnp.zeros_like(query_key_value_bias), qkv_bias_own, t * width, 1
    )
    fc1_slot = lax.dynamic_update_slice_in_dim(
        jnp.zeros_like(fc1_bias), fc1_bias_own, t * units, 0
    )
    smalls = [
        gain_one,
        shift_one,
        qkv_slot,
        out_bias_part,
        gain_two,
        shift_two,
        fc1_slot,
        fc2_bias_part,
    ]
    packed = net.total(jnp.concatenate([part.reshape(-1) for part in smalls]))
    done, at = [], 0
    for part in smalls:
        done.append(packed[at : at + part.size].reshape(part.shape))
        at += part.size
    gain_one, shift_one, qkv_slot, out_bias_g, gain_two, shift_two, fc1_slot, fc2_bias_g = done
    return (
        block_out,
        grad_input,
        gain_one,
        shift_one,
        jnp.concatenate([dw_q, dw_k, dw_v], axis=1).reshape(rows, 3, width),
        qkv_slot,
        dout.T,
        out_bias_g,
        gain_two,
        shift_two,
        jnp.concatenate([dfc1_a, dfc1_b], axis=1),
        fc1_slot,
        jnp.concatenate([dfc2_a, dfc2_b], axis=1).T,
        fc2_bias_g,
    )


def solution(mesh):
    tokens = P(("shard", "tensor"), "context", None)
    rows_split = P(("shard", "context"), "tensor")
    columns_split = P("tensor", ("shard", "context"))
    qkv_split = P(("shard", "context"), None, "tensor")
    places = P("shard", "context")
    return jax.shard_map(
        functools.partial(on_device, mesh.shape["shard"]),
        mesh=mesh,
        in_specs=(
            tokens, places, places, P(), P(), qkv_split, P(), columns_split, P(),
            P(), P(), rows_split, P(), columns_split, P(), tokens,
        ),
        out_specs=(
            tokens, tokens, P(), P(), qkv_split, P(), columns_split, P(), P(), P(),
            rows_split, P(), columns_split, P(),
        ),
        check_vma=False,
    )
```
